32 devices in a mesh: lat: 8 (over z, y), lon: 4 (over x, core).
Axes of the slice: x: 2, y: 2, z: 4, core: 2. Of those that a mesh axis runs over, the one named last changes fastest.
Arguments:
- features: bfloat16 [98304, 128], P(('lat', 'lon')), may hold values from -6 to 6
- cell_index: int32 [98304], P(('lat', 'lon')), may hold values from 0 to 2547
- tile_rows: int32 [1024], P(('lat', 'lon')), may hold values from 1 to 96, as said below
- spread: float32 [3, 3], replicated, may hold values from 0.2 to 1
- w_in: bfloat16 [128, 256], replicated, may hold values from -0.5 to 0.5
- w_dens: float32 [256], replicated, may hold values from -3 to 3
- w_one: bfloat16 [3, 3, 256, 256], replicated, may hold values from -0.125 to 0.125
- w_two: bfloat16 [3, 3, 256, 256], replicated, may hold values from -0.125 to 0.125
Outputs:
- encoded: bfloat16 [192, 384, 256], P('lat', 'lon')
The draws below stay inside these ranges and needn't reach their ends.
Inputs may be any that keep to these rules, and one draw needn't show every extreme that they name: `tile_rows`: every block has 1 to 96 used slots; on every device some block has exactly 96.
All inputs are finite; a program needn't handle non-finite values.
Results may differ from the reference program's by a relative error of at most 0.0054.
Values may be sent and summed in bfloat16 or wider, within the bound.
A program may use at most 64 MiB of HBM per device.

```python
import math
import jax
import jax.numpy as jnp
from jax import lax

TH = 24
TW = 96
F = 128
C = 256
CAP = 96
TILES = 32
OBS_ALL = 98304
PH = 26
PW = 98
GH = 192
GW = 384
N_LAT = 8
N_LON = 4
DEVICES = 32


def draw_tile_rows(key, part):
    heat = jax.random.randint(jax.random.fold_in(key, 11), (TILES,), 1, 5)
    low = jnp.maximum(1, heat * CAP // 8)
    high = heat * CAP // 4 + 1
    counts = jax.random.randint(jax.random.fold_in(key, 12), (DEVICES, TILES), low[None, :], high[None, :])
    counts = jnp.minimum(counts, CAP)
    forced = jax.random.randint(jax.random.fold_in(key, 13), (DEVICES,), 0, TILES)
    tile_ids = jnp.arange(TILES, dtype=jnp.int32)
    counts = jnp.where(tile_ids[None, :] == forced[:, None], CAP, counts)
    return counts.reshape(DEVICES * TILES).astype(jnp.int32)


def with_ends(entries, own_key, smallest, largest):
    longest = entries.shape.index(max(entries.shape))
    spots = []
    for shift in (0, 1):
        where = [jax.random.randint(jax.random.fold_in(own_key, axis), (), 0, length) for axis, length in enumerate(entries.shape)]
        where[longest] = (where[longest] + shift) % entries.shape[longest]
        spots.append(tuple(where))
    return entries.at[spots[0]].set(smallest).at[spots[1]].set(largest)


def level_of(key, extent, cuts, low, high):
    gain, own = 1.0, jax.random.fold_in(key, 6)
    for position, blocks in cuts:
        steps = jnp.exp(jax.random.uniform(jax.random.fold_in(own, position), (blocks,), jnp.float32, low / len(cuts), high / len(cuts)))
        gain = gain * jnp.repeat(steps, extent[position] // blocks).reshape([-1 if axis == position else 1 for axis in range(len(extent))])
    return gain


def bell_draw(key, shape, scale, limit, cuts=(), held_as=jnp.bfloat16):
    values = jax.random.normal(key, shape, jnp.float32) * scale
    if len(cuts) > 0:
        values = level_of(key, shape, cuts, -0.22, 0.18) * values
    return jnp.clip(values, min=-limit, max=limit).astype(held_as)


def setup_inputs(seed: int = 0) -> dict:
    seeds = jax.random.split(jax.random.key(seed), 9)
    return {
        "features": bell_draw(seeds[0], (OBS_ALL, F), 1.0, 6.0, ((0, 32),)),
        "cell_index": with_ends(jax.random.randint(seeds[1], (OBS_ALL,), 0, PH * PW), jax.random.fold_in(seeds[1], 1), 0, (PH * PW) - 1).astype(jnp.int32),
        "tile_rows": draw_tile_rows(jax.random.fold_in(seeds[8], 71), 0),
        "spread": jnp.clip(jnp.exp(jax.random.uniform(seeds[3], (3, 3), jnp.float32, math.log(0.2), math.log(1.0))), 0.2, 1.0),
        "w_in": bell_draw(seeds[4], (F, C), F ** -0.5, 0.5),
        "w_dens": bell_draw(seeds[5], (C,), 0.5, 3.0, (), jnp.float32),
        "w_one": bell_draw(seeds[6], (3, 3, C, C), (9 * C) ** -0.5, 0.125),
        "w_two": bell_draw(seeds[7], (3, 3, C, C), (9 * C) ** -0.5, 0.125),
    }


def wrap_pad(field):
    cols = jnp.concatenate([field[:, -1:], field, field[:, :1]], axis=1)
    return jnp.pad(cols, ((1, 1), (0, 0), (0, 0)))


def conv_grid(field, weight):
    padded = wrap_pad(field)
    rows_all, cols_all, chans = field.shape
    total = jnp.zeros((rows_all * cols_all, weight.shape[3]), jnp.float32)
    for row_off in range(3):
        for col_off in range(3):
            window = padded[row_off:row_off + rows_all, col_off:col_off + cols_all].reshape(-1, chans)
            total = total + jnp.dot(window, weight[row_off, col_off], preferred_element_type=jnp.float32)
    return total.reshape(rows_all, cols_all, -1)


def reference(features, cell_index, tile_rows, spread, w_in, w_dens, w_one, w_two):
    tiles = N_LAT * N_LON
    frame_cells = PH * PW
    blocks = features.reshape(DEVICES, tiles, CAP, F)
    cell_blocks = cell_index.reshape(DEVICES, tiles, CAP)
    counts = tile_rows.reshape(DEVICES, tiles)
    slot_ids = jnp.arange(CAP, dtype=jnp.int32)

    def one_tile(tile):
        rows = lax.dynamic_index_in_dim(blocks, tile, 1, keepdims=False)
        cells = lax.dynamic_index_in_dim(cell_blocks, tile, 1, keepdims=False)
        used = lax.dynamic_index_in_dim(counts, tile, 1, keepdims=False)
        valid = slot_ids[None, :] < used[:, None]
        segment = jnp.where(valid, cells, frame_cells).reshape(-1).astype(jnp.int32)
        sums = jax.ops.segment_sum(rows.reshape(-1, F).astype(jnp.float32), segment, num_segments=frame_cells + 1)
        numbers = jax.ops.segment_sum(jnp.ones(segment.shape, jnp.float32), segment, num_segments=frame_cells + 1)
        return sums[:frame_cells], numbers[:frame_cells]

    frame_sum, frame_count = lax.map(one_tile, jnp.arange(tiles, dtype=jnp.int32))
    frame_sum = frame_sum.reshape(tiles, PH, PW, F)
    frame_count = frame_count.reshape(tiles, PH, PW)
    data = jnp.zeros((tiles, TH, TW, F), jnp.float32)
    density = jnp.zeros((tiles, TH, TW), jnp.float32)
    for row_off in range(3):
        for col_off in range(3):
            data = data + spread[row_off, col_off] * frame_sum[:, row_off:row_off + TH, col_off:col_off + TW]
            density = density + spread[row_off, col_off] * frame_count[:, row_off:row_off + TH, col_off:col_off + TW]
    mean = (data / (1.0 + density)[..., None]).astype(jnp.bfloat16)
    grid = jnp.dot(mean.reshape(-1, F), w_in, preferred_element_type=jnp.float32)
    grid = grid + jnp.log1p(density).reshape(-1, 1) * w_dens[None, :]
    grid = grid.astype(jnp.bfloat16).reshape(N_LAT, N_LON, TH, TW, C)
    grid = jnp.transpose(grid, (0, 2, 1, 3, 4)).reshape(GH, GW, C)
    hidden = jax.nn.silu(conv_grid(grid, w_one)).astype(jnp.bfloat16)
    encoded = grid.astype(jnp.float32) + conv_grid(hidden, w_two)
    return encoded.astype(jnp.bfloat16)
```

```python
import functools

import jax
import jax.numpy as jnp
from jax import lax
from jax.experimental import pallas as pl
from jax.experimental.pallas import tpu as pltpu
from jax.sharding import PartitionSpec as P

TH = 24
TW = 96
F = 128
C = 256
CAP = 96
PH = 26
PW = 98
PWP = 112
GROUP = 8
HALF = PH // 2
ROWS = 8
MESH = pl.DeviceIdType.MESH
F32 = jnp.float32
BF16 = jnp.bfloat16


def xor(a, b, count):
    out = 0
    bit = 1
    while bit < count:
        out = out + ((a // bit + b // bit) % 2) * bit
        bit *= 2
    return out


def kernel(
    lat_n, lon_n,
    feats, cells, spread, w_in, w_dens, w_one, w_two, out,
    rows_in, cells_in, lhs, acc, mean, logd, grid_x, hid_x, win_v, wone_v, wtwo_v,
    row_out, row_in, col_out, col_in, corner_in,
    row_send, row_recv, cell_send, cell_recv, own_sem, w_sem, halo_send, halo_recv,
):
    n = lat_n * lon_n
    groups = n // GROUP
    lat = lax.axis_index("lat")
    lon = lax.axis_index("lon")
    me = lat * lon_n + lon
    my_group = me // GROUP
    my_place = me % GROUP
    east = (lon + 1) % lon_n
    west = (lon + lon_n - 1) % lon_n

    barrier = pltpu.get_barrier_semaphore()

    @pl.loop(1, n)
    def _(k):
        peer = (me + k) % n
        pl.semaphore_signal(
            barrier, inc=1, device_id=(peer // lon_n, peer % lon_n), device_id_type=MESH
        )

    own = [
        pltpu.make_async_copy(feats.at[me], rows_in.at[me], own_sem.at[0]),
        pltpu.make_async_copy(cells.at[me], cells_in.at[me], own_sem.at[1]),
    ]
    weights = [
        pltpu.make_async_copy(w_in, win_v, w_sem.at[0]),
        pltpu.make_async_copy(w_one, wone_v, w_sem.at[1]),
        pltpu.make_async_copy(w_two, wtwo_v, w_sem.at[2]),
    ]
    for item in own + weights:
        item.start()
    pl.semaphore_wait(barrier, n - 1)

    def row_copy(src_block, slot, peer):
        return pltpu.make_async_remote_copy(
            src_ref=feats.at[src_block], dst_ref=rows_in.at[slot],
            send_sem=row_send.at[src_block], recv_sem=row_recv.at[slot],
            device_id=(peer // lon_n, peer % lon_n), device_id_type=MESH,
        )

    def cell_copy(src_block, slot, peer):
        return pltpu.make_async_remote_copy(
            src_ref=cells.at[src_block], dst_ref=cells_in.at[slot],
            send_sem=cell_send.at[src_block], recv_sem=cell_recv.at[slot],
            device_id=(peer // lon_n, peer % lon_n), device_id_type=MESH,
        )

    def peer_of(step):
        turn = groups - 1 - step // GROUP
        return xor(my_group, turn, groups) * GROUP + (my_place + step % GROUP) % GROUP

    def each_peer(act):
        @pl.loop(0, n - GROUP)
        def _(step):
            act(peer_of(step))

        for place in range(1, GROUP):
            act(my_group * GROUP + (my_place + place) % GROUP)

    def send(peer):
        cell_copy(peer, me, peer).start()
        row_copy(peer, me, peer).start()

    each_peer(send)

    acc[...] = jnp.zeros_like(acc)

    def add_group(base):
        enc = jnp.concatenate([cells_in[base + m][:, :CAP] for m in range(GROUP)], axis=1)
        wide = GROUP * CAP
        col = jnp.broadcast_to(enc & 127, (PWP, wide))
        col_hot = jnp.where(
            lax.broadcasted_iota(jnp.int32, (PWP, wide), 0) == col, 1.0, 0.0
        ).astype(BF16)
        row = jnp.broadcast_to(enc >> 7, (16, wide))
        rows = rows_in[pl.ds(base, GROUP)].reshape(wide, F)
        rhs = jnp.concatenate([rows, jnp.ones((wide, C - F), BF16)], axis=1)
        col_hot = col_hot.reshape(PWP // 16, 16, wide)
        for r in range(PH):
            here = jnp.where(row == r, 1.0, 0.0).astype(BF16)
            lhs[r] = (col_hot * here[None]).reshape(PWP, wide)
        for half in range(2):
            span = slice(half * HALF, (half + 1) * HALF)
            part = jnp.dot(
                lhs[span].reshape(HALF * PWP, wide), rhs, preferred_element_type=F32
            )
            acc[span] += part.reshape(HALF, PWP, C)

    @pl.loop(0, groups - 1)
    def _(step):
        base = xor(my_group, groups - 1 - step, groups) * GROUP
        for m in range(GROUP):
            cell_copy(base + m, base + m, base + m).wait_recv()
            row_copy(base + m, base + m, base + m).wait_recv()
        add_group(base)

    for place in range(1, GROUP):
        peer = my_group * GROUP + (my_place + place) % GROUP
        cell_copy(peer, peer, peer).wait_recv()
        row_copy(peer, peer, peer).wait_recv()
    for item in own:
        item.wait()
    add_group(my_group * GROUP)

    weights[0].wait()

    def put(x_ref, stage, r, value):
        x_ref[r + 1, :, C : 2 * C] = value.astype(BF16)
        x_ref[r + 1, :, 0:C] = pltpu.roll(value, 1, 0).astype(BF16)
        x_ref[r + 1, :, 2 * C :] = pltpu.roll(value, TW - 1, 0).astype(BF16)
        col_out[stage, 0, pl.ds(r, 1)] = value[0:1]
        col_out[stage, 1, pl.ds(r, 1)] = value[TW - 1 : TW]

    @pl.loop(0, TH)
    def _(r):
        parts = []
        for b in range(3):
            parts.append(
                sum(spread[a, b] * acc[r + a, 0:104] for a in range(3))
            )
        total = parts[0][0:TW] + parts[1][1 : TW + 1] + parts[2][2 : TW + 2]
        level = 1.0 + total[:, F:]
        mean[r] = (total[:, :F] / level).astype(BF16)
        logd[r] = jnp.log(level)

    @pl.loop(0, TH // ROWS)
    def _(step):
        start = step * ROWS
        grid = jnp.dot(
            mean[pl.ds(start, ROWS)].reshape(ROWS * TW, F), win_v[...],
            preferred_element_type=F32,
        ).reshape(ROWS, TW, C)
        for k in range(ROWS):
            lg = logd[start + k]
            value = grid[k] + jnp.concatenate([lg, lg], axis=1) * w_dens[...]
            put(grid_x, 0, start + k, value)

    def halo_copy(stage, kind, src, dst, where):
        return pltpu.make_async_remote_copy(
            src_ref=src, dst_ref=dst,
            send_sem=halo_send.at[stage, kind], recv_sem=halo_recv.at[stage, kind],
            device_id=where, device_id_type=MESH,
        )

    def copies(stage, x_ref):
        up, down = lat - 1, lat + 1
        left, right = col_out.at[stage, 0], col_out.at[stage, 1]
        both = [
            halo_copy(stage, 0, right, col_in.at[stage, 0], (lat, east)),
            halo_copy(stage, 1, left, col_in.at[stage, 1], (lat, west)),
        ]
        low, high = pl.ds(0, 8), pl.ds(TH - 8, 8)
        to_up = [
            halo_copy(stage, 2, row_out.at[stage, 0], row_in.at[stage, 1], (up, lon)),
            halo_copy(stage, 3, right.at[low], corner_in.at[stage, 2], (up, east)),
            halo_copy(stage, 4, left.at[low], corner_in.at[stage, 3], (up, west)),
        ]
        to_down = [
            halo_copy(stage, 5, row_out.at[stage, 1], row_in.at[stage, 0], (down, lon)),
            halo_copy(stage, 6, right.at[high], corner_in.at[stage, 0], (down, east)),
            halo_copy(stage, 7, left.at[high], corner_in.at[stage, 1], (down, west)),
        ]
        return both, to_up, to_down

    def set_edges(x_ref, r, left, right):
        ids = lax.broadcasted_iota(jnp.int32, (16, C), 0)
        first = x_ref[r, 0:16, 0:C].astype(F32)
        x_ref[r, 0:16, 0:C] = jnp.where(ids == 0, left, first).astype(BF16)
        last = x_ref[r, TW - 16 : TW, 2 * C :].astype(F32)
        x_ref[r, TW - 16 : TW, 2 * C :] = jnp.where(ids == 15, right, last).astype(BF16)

    def exchange(stage, x_ref):
        row_out[stage, 0] = x_ref[1, :, C : 2 * C]
        row_out[stage, 1] = x_ref[TH, :, C : 2 * C]
        both, to_up, to_down = copies(stage, x_ref)
        for item in both:
            item.start()

        @pl.when(lat > 0)
        def _():
            for item in to_up:
                item.start()

        @pl.when(lat < lat_n - 1)
        def _():
            for item in to_down:
                item.start()

        for item in both:
            item.wait_recv()

        @pl.loop(0, TH)
        def _(r):
            set_edges(
                x_ref, r + 1, col_in[stage, 0, pl.ds(r, 1)], col_in[stage, 1, pl.ds(r, 1)]
            )

        def outer(r, side, corner_row):
            value = row_in[stage, side].astype(F32)
            x_ref[r, :, C : 2 * C] = row_in[stage, side]
            x_ref[r, :, 0:C] = pltpu.roll(value, 1, 0).astype(BF16)
            x_ref[r, :, 2 * C :] = pltpu.roll(value, TW - 1, 0).astype(BF16)
            rows = slice(corner_row, corner_row + 1)
            set_edges(
                x_ref, r, corner_in[stage, 2 * side, rows], corner_in[stage, 2 * side + 1, rows]
            )

        @pl.when(lat > 0)
        def _():
            for item in to_down:
                item.wait_recv()
            outer(0, 0, 7)

        @pl.when(lat == 0)
        def _():
            x_ref[0] = jnp.zeros((TW, 3 * C), BF16)

        @pl.when(lat < lat_n - 1)
        def _():
            for item in to_up:
                item.wait_recv()
            outer(TH + 1, 1, 0)

        @pl.when(lat == lat_n - 1)
        def _():
            x_ref[TH + 1] = jnp.zeros((TW, 3 * C), BF16)

        for item in both:
            item.wait_send()

        @pl.when(lat > 0)
        def _():
            for item in to_up:
                item.wait_send()

        @pl.when(lat < lat_n - 1)
        def _():
            for item in to_down:
                item.wait_send()

    def conv(x_ref, weight, start):
        window = jnp.concatenate(
            [x_ref[pl.ds(start + a, ROWS)].reshape(ROWS * TW, 3 * C) for a in range(3)], axis=1
        )
        return jnp.dot(window, weight[...], preferred_element_type=F32).reshape(ROWS, TW, C)

    exchange(0, grid_x)
    weights[1].wait()

    @pl.loop(0, TH // ROWS)
    def _(step):
        start = step * ROWS
        total = conv(grid_x, wone_v, start)
        for k in range(ROWS):
            value = total[k]
            put(hid_x, 1, start + k, value / (1.0 + jnp.exp(-value)))

    exchange(1, hid_x)
    weights[2].wait()

    @pl.loop(0, TH // ROWS)
    def _(step):
        start = step * ROWS
        total = conv(hid_x, wtwo_v, start)
        base = grid_x[pl.ds(start + 1, ROWS), :, C : 2 * C].astype(F32)
        out[pl.ds(start, ROWS)] = (base + total).astype(BF16)

    def sent(peer):
        cell_copy(peer, me, peer).wait_send()
        row_copy(peer, me, peer).wait_send()

    each_peer(sent)


def shards(features, cell_index, tile_rows, spread, w_in, w_dens, w_one, w_two):
    lat_n = lax.axis_size("lat")
    lon_n = lax.axis_size("lon")
    n = lat_n * lon_n
    cell = cell_index.reshape(n, CAP)
    used = jnp.arange(CAP, dtype=jnp.int32)[None, :] < tile_rows[:, None]
    code = jnp.where(used, (cell // PW) * 128 + cell % PW, 127 * 128)
    code = jnp.pad(code, ((0, 0), (0, 128 - CAP))).reshape(n, 1, 128)
    anywhere = pl.BlockSpec(memory_space=pl.ANY)
    vmem = pl.BlockSpec(memory_space=pltpu.VMEM)
    smem = pl.BlockSpec(memory_space=pltpu.SMEM)
    dma = pltpu.SemaphoreType.DMA
    return pl.pallas_call(
        functools.partial(kernel, lat_n, lon_n),
        out_shape=jax.ShapeDtypeStruct((TH, TW, C), BF16),
        in_specs=[anywhere, anywhere, smem, anywhere, vmem, anywhere, anywhere],
        out_specs=vmem,
        scratch_shapes=[
            pltpu.VMEM((n, CAP, F), BF16),
            pltpu.VMEM((n, 1, 128), jnp.int32),
            pltpu.VMEM((PH, PWP, GROUP * CAP), BF16),
            pltpu.VMEM((PH, PWP, C), F32),
            pltpu.VMEM((TH, TW, F), BF16),
            pltpu.VMEM((TH, TW, F), F32),
            pltpu.VMEM((TH + 2, TW, 3 * C), BF16),
            pltpu.VMEM((TH + 2, TW, 3 * C), BF16),
            pltpu.VMEM((F, C), BF16),
            pltpu.VMEM((9 * C, C), BF16),
            pltpu.VMEM((9 * C, C), BF16),
            pltpu.VMEM((2, 2, TW, C), BF16),
            pltpu.VMEM((2, 2, TW, C), BF16),
            pltpu.VMEM((2, 2, TH, C), F32),
            pltpu.VMEM((2, 2, TH, C), F32),
            pltpu.VMEM((2, 4, 8, C), F32),
            dma((n,)), dma((n,)), dma((n,)), dma((n,)),
            dma((2,)), dma((3,)), dma((2, 8)), dma((2, 8)),
        ],
        compiler_params=pltpu.CompilerParams(
            collective_id=0, has_side_effects=True, vmem_limit_bytes=60 * 1024 * 1024
        ),
    )(
        features.reshape(n, CAP, F), code, spread, w_in, w_dens.reshape(1, C),
        w_one.reshape(9 * C, C), w_two.reshape(9 * C, C),
    )


def solution(mesh):
    blocks = P(("lat", "lon"))
    in_specs = (P(("lat", "lon"), None), blocks, blocks, P(), P(), P(), P(), P())
    out_specs = P("lat", "lon", None)
    return jax.shard_map(shards, mesh=mesh, in_specs=in_specs, out_specs=out_specs, check_vma=False)
```

```python
import functools

import jax
import jax.numpy as jnp
from jax import lax
from jax.experimental import pallas as pl
from jax.experimental.pallas import tpu as pltpu
from jax.sharding import PartitionSpec as P

TH = 24
TW = 96
F = 128
C = 256
CAP = 96
PH = 26
PW = 98
PWP = 112
GROUP = 8
HALF = PH // 2
ROWS = 8
MESH = pl.DeviceIdType.MESH
F32 = jnp.float32
BF16 = jnp.bfloat16


def xor(a, b, count):
    out = 0
    bit = 1
    while bit < count:
        out = out + ((a // bit + b // bit) % 2) * bit
        bit *= 2
    return out


def kernel(
    lat_n, lon_n,
    feats, raw, used, spread, w_in, w_dens, w_one, w_two, out,
    cells, out_v, rows_in, cells_in, lhs, acc, mean, logd, grid_x, hid_x, win_v, wone_v, wtwo_v,
    row_out, row_in, col_out, col_in, corner_in,
    row_send, row_recv, cell_send, cell_recv, own_sem, w_sem, out_sem, halo_send, halo_recv,
):
    n = lat_n * lon_n
    groups = n // GROUP
    lat = lax.axis_index("lat")
    lon = lax.axis_index("lon")
    me = lat * lon_n + lon
    my_group = me // GROUP
    my_place = me % GROUP
    east = (lon + 1) % lon_n
    west = (lon + lon_n - 1) % lon_n

    barrier = pltpu.get_barrier_semaphore()

    @pl.loop(1, n)
    def _(k):
        peer = (me + k) % n
        pl.semaphore_signal(
            barrier, inc=1, device_id=(peer // lon_n, peer % lon_n), device_id_type=MESH
        )

    lane = lax.broadcasted_iota(jnp.int32, (1, 128), 1)

    @pl.loop(0, n // 4)
    def _(quad):
        one, two, three = (raw[pl.ds(3 * quad + k, 1)] for k in range(3))
        picks = [
            one,
            jnp.where(lane < 32, pltpu.roll(one, 32, 1), pltpu.roll(two, 32, 1)),
            jnp.where(lane < 64, pltpu.roll(two, 64, 1), pltpu.roll(three, 64, 1)),
            pltpu.roll(three, 96, 1),
        ]
        for k, pick in enumerate(picks):
            row = ((pick.astype(F32) + 0.5) * (1.0 / PW)).astype(jnp.int32)
            code = row * 128 + (pick - row * PW)
            cells[4 * quad + k] = jnp.where(lane < used[4 * quad + k], code, 127 * 128)

    own = [
        pltpu.make_async_copy(feats.at[me], rows_in.at[me], own_sem.at[0]),
        pltpu.make_async_copy(cells.at[me], cells_in.at[me], own_sem.at[1]),
    ]
    weights = [
        pltpu.make_async_copy(w_in, win_v, w_sem.at[0]),
        pltpu.make_async_copy(w_one, wone_v, w_sem.at[1]),
        pltpu.make_async_copy(w_two, wtwo_v, w_sem.at[2]),
    ]
    for item in weights:
        item.start()
    pl.semaphore_wait(barrier, n - 1)

    def row_copy(src_block, slot, peer):
        return pltpu.make_async_remote_copy(
            src_ref=feats.at[src_block], dst_ref=rows_in.at[slot],
            send_sem=row_send.at[src_block], recv_sem=row_recv.at[slot],
            device_id=(peer // lon_n, peer % lon_n), device_id_type=MESH,
        )

    def cell_copy(src_block, slot, peer):
        return pltpu.make_async_remote_copy(
            src_ref=cells.at[src_block], dst_ref=cells_in.at[slot],
            send_sem=cell_send.at[src_block], recv_sem=cell_recv.at[slot],
            device_id=(peer // lon_n, peer % lon_n), device_id_type=MESH,
        )

    def peer_of(step):
        turn = 1 + step // GROUP
        return xor(my_group, turn, groups) * GROUP + (my_place + step % GROUP) % GROUP

    def each_peer(act):
        for place in range(1, GROUP):
            act(my_group * GROUP + (my_place + place) % GROUP)

        @pl.loop(0, n - GROUP)
        def _(step):
            act(peer_of(step))

    def send(peer):
        cell_copy(peer, me, peer).start()
        row_copy(peer, me, peer).start()

    each_peer(send)
    for item in own:
        item.start()

    acc[...] = jnp.zeros_like(acc)

    def add_group(base):
        enc = jnp.concatenate([cells_in[base + m][:, :CAP] for m in range(GROUP)], axis=1)
        wide = GROUP * CAP
        col = jnp.broadcast_to(enc & 127, (PWP, wide))
        col_hot = jnp.where(
            lax.broadcasted_iota(jnp.int32, (PWP, wide), 0) == col, 1.0, 0.0
        ).astype(BF16)
        row = jnp.broadcast_to(enc >> 7, (16, wide))
        rows = rows_in[pl.ds(base, GROUP)].reshape(wide, F)
        rhs = jnp.concatenate([rows, jnp.ones((wide, C - F), BF16)], axis=1)
        col_hot = col_hot.reshape(PWP // 16, 16, wide)
        for r in range(PH):
            here = jnp.where(row == r, 1.0, 0.0).astype(BF16)
            lhs[r] = (col_hot * here[None]).reshape(PWP, wide)
        for half in range(2):
            span = slice(half * HALF, (half + 1) * HALF)
            part = jnp.dot(
                lhs[span].reshape(HALF * PWP, wide), rhs, preferred_element_type=F32
            )
            acc[span] += part.reshape(HALF, PWP, C)

    for place in range(1, GROUP):
        peer = my_group * GROUP + (my_place + place) % GROUP
        cell_copy(peer, peer, peer).wait_recv()
        row_copy(peer, peer, peer).wait_recv()
    for item in own:
        item.wait()
    add_group(my_group * GROUP)

    @pl.loop(1, groups)
    def _(step):
        base = xor(my_group, step, groups) * GROUP
        for m in range(GROUP):
            cell_copy(base + m, base + m, base + m).wait_recv()
            row_copy(base + m, base + m, base + m).wait_recv()
        add_group(base)

    weights[0].wait()

    def put(x_ref, stage, r, value):
        x_ref[r + 1, :, C : 2 * C] = value.astype(BF16)
        x_ref[r + 1, :, 0:C] = pltpu.roll(value, 1, 0).astype(BF16)
        x_ref[r + 1, :, 2 * C :] = pltpu.roll(value, TW - 1, 0).astype(BF16)
        col_out[stage, 0, pl.ds(r, 1)] = value[0:1]
        col_out[stage, 1, pl.ds(r, 1)] = value[TW - 1 : TW]

    @pl.loop(0, TH)
    def _(r):
        parts = []
        for b in range(3):
            parts.append(
                sum(spread[a, b] * acc[r + a, 0:104] for a in range(3))
            )
        total = parts[0][0:TW] + parts[1][1 : TW + 1] + parts[2][2 : TW + 2]
        level = 1.0 + total[:, F:]
        mean[r] = (total[:, :F] / level).astype(BF16)
        logd[r] = jnp.log(level)

    @pl.loop(0, TH // ROWS)
    def _(step):
        start = step * ROWS
        grid = jnp.dot(
            mean[pl.ds(start, ROWS)].reshape(ROWS * TW, F), win_v[...],
            preferred_element_type=F32,
        ).reshape(ROWS, TW, C)
        for k in range(ROWS):
            lg = logd[start + k]
            value = grid[k] + jnp.concatenate([lg, lg], axis=1) * w_dens[...]
            put(grid_x, 0, start + k, value)

    def halo_copy(stage, kind, src, dst, where):
        return pltpu.make_async_remote_copy(
            src_ref=src, dst_ref=dst,
            send_sem=halo_send.at[stage, kind], recv_sem=halo_recv.at[stage, kind],
            device_id=where, device_id_type=MESH,
        )

    def copies(stage, x_ref):
        up, down = lat - 1, lat + 1
        left, right = col_out.at[stage, 0], col_out.at[stage, 1]
        both = [
            halo_copy(stage, 0, right, col_in.at[stage, 0], (lat, east)),
            halo_copy(stage, 1, left, col_in.at[stage, 1], (lat, west)),
        ]
        low, high = pl.ds(0, 8), pl.ds(TH - 8, 8)
        to_up = [
            halo_copy(stage, 2, row_out.at[stage, 0], row_in.at[stage, 1], (up, lon)),
            halo_copy(stage, 3, right.at[low], corner_in.at[stage, 2], (up, east)),
            halo_copy(stage, 4, left.at[low], corner_in.at[stage, 3], (up, west)),
        ]
        to_down = [
            halo_copy(stage, 5, row_out.at[stage, 1], row_in.at[stage, 0], (down, lon)),
            halo_copy(stage, 6, right.at[high], corner_in.at[stage, 0], (down, east)),
            halo_copy(stage, 7, left.at[high], corner_in.at[stage, 1], (down, west)),
        ]
        return both, to_up, to_down

    def set_edges(x_ref, r, left, right):
        ids = lax.broadcasted_iota(jnp.int32, (16, C), 0)
        first = x_ref[r, 0:16, 0:C].astype(F32)
        x_ref[r, 0:16, 0:C] = jnp.where(ids == 0, left, first).astype(BF16)
        last = x_ref[r, TW - 16 : TW, 2 * C :].astype(F32)
        x_ref[r, TW - 16 : TW, 2 * C :] = jnp.where(ids == 15, right, last).astype(BF16)

    def exchange(stage, x_ref, beside):
        row_out[stage, 0] = x_ref[1, :, C : 2 * C]
        row_out[stage, 1] = x_ref[TH, :, C : 2 * C]
        both, to_up, to_down = copies(stage, x_ref)
        for item in both:
            item.start()

        @pl.when(lat > 0)
        def _():
            for item in to_up:
                item.start()

        @pl.when(lat < lat_n - 1)
        def _():
            for item in to_down:
                item.start()

        beside()
        for item in both:
            item.wait_recv()

        @pl.loop(0, TH, unroll=4)
        def _(r):
            set_edges(
                x_ref, r + 1, col_in[stage, 0, pl.ds(r, 1)], col_in[stage, 1, pl.ds(r, 1)]
            )

        def outer(r, side, corner_row):
            value = row_in[stage, side].astype(F32)
            x_ref[r, :, C : 2 * C] = row_in[stage, side]
            x_ref[r, :, 0:C] = pltpu.roll(value, 1, 0).astype(BF16)
            x_ref[r, :, 2 * C :] = pltpu.roll(value, TW - 1, 0).astype(BF16)
            rows = slice(corner_row, corner_row + 1)
            set_edges(
                x_ref, r, corner_in[stage, 2 * side, rows], corner_in[stage, 2 * side + 1, rows]
            )

        @pl.when(lat > 0)
        def _():
            for item in to_down:
                item.wait_recv()
            outer(0, 0, 7)

        @pl.when(lat == 0)
        def _():
            x_ref[0] = jnp.zeros((TW, 3 * C), BF16)

        @pl.when(lat < lat_n - 1)
        def _():
            for item in to_up:
                item.wait_recv()
            outer(TH + 1, 1, 0)

        @pl.when(lat == lat_n - 1)
        def _():
            x_ref[TH + 1] = jnp.zeros((TW, 3 * C), BF16)

        for item in both:
            item.wait_send()

        @pl.when(lat > 0)
        def _():
            for item in to_up:
                item.wait_send()

        @pl.when(lat < lat_n - 1)
        def _():
            for item in to_down:
                item.wait_send()

    def conv(x_ref, weight, start):
        window = jnp.concatenate(
            [x_ref[pl.ds(start + a, ROWS)].reshape(ROWS * TW, 3 * C) for a in range(3)], axis=1
        )
        return jnp.dot(window, weight[...], preferred_element_type=F32).reshape(ROWS, TW, C)

    def sent(peer):
        cell_copy(peer, me, peer).wait_send()
        row_copy(peer, me, peer).wait_send()

    exchange(0, grid_x, lambda: each_peer(sent))
    weights[1].wait()

    @pl.loop(0, TH // ROWS)
    def _(step):
        start = step * ROWS
        total = conv(grid_x, wone_v, start)
        for k in range(ROWS):
            value = total[k]
            put(hid_x, 1, start + k, value / (1.0 + jnp.exp(-value)))

    exchange(1, hid_x, lambda: None)
    weights[2].wait()

    def out_copy(start):
        span = pl.ds(start, ROWS)
        return pltpu.make_async_copy(out_v.at[span], out.at[span], out_sem.at[start // ROWS])

    @pl.loop(0, TH // ROWS)
    def _(step):
        start = step * ROWS
        total = conv(hid_x, wtwo_v, start)
        base = grid_x[pl.ds(start + 1, ROWS), :, C : 2 * C].astype(F32)
        out_v[pl.ds(start, ROWS)] = (base + total).astype(BF16)
        out_copy(start).start()

    for step in range(TH // ROWS):
        out_copy(step * ROWS).wait()


def shards(features, cell_index, tile_rows, spread, w_in, w_dens, w_one, w_two):
    lat_n = lax.axis_size("lat")
    lon_n = lax.axis_size("lon")
    n = lat_n * lon_n
    hbm = pl.BlockSpec(memory_space=pltpu.HBM)
    anywhere = pl.BlockSpec(memory_space=pl.ANY)
    vmem = pl.BlockSpec(memory_space=pltpu.VMEM)
    smem = pl.BlockSpec(memory_space=pltpu.SMEM)
    dma = pltpu.SemaphoreType.DMA
    return pl.pallas_call(
        functools.partial(kernel, lat_n, lon_n),
        out_shape=jax.ShapeDtypeStruct((TH, TW, C), BF16),
        in_specs=[hbm, vmem, smem, smem, hbm, vmem, hbm, hbm],
        out_specs=anywhere,
        scratch_shapes=[
            pltpu.VMEM((n, 1, 128), jnp.int32),
            pltpu.VMEM((TH, TW, C), BF16),
            pltpu.VMEM((n, CAP, F), BF16),
            pltpu.VMEM((n, 1, 128), jnp.int32),
            pltpu.VMEM((PH, PWP, GROUP * CAP), BF16),
            pltpu.VMEM((PH, PWP, C), F32),
            pltpu.VMEM((TH, TW, F), BF16),
            pltpu.VMEM((TH, TW, F), F32),
            pltpu.VMEM((TH + 2, TW, 3 * C), BF16),
            pltpu.VMEM((TH + 2, TW, 3 * C), BF16),
            pltpu.VMEM((F, C), BF16),
            pltpu.VMEM((9 * C, C), BF16),
            pltpu.VMEM((9 * C, C), BF16),
            pltpu.VMEM((2, 2, TW, C), BF16),
            pltpu.VMEM((2, 2, TW, C), BF16),
            pltpu.VMEM((2, 2, TH, C), F32),
            pltpu.VMEM((2, 2, TH, C), F32),
            pltpu.VMEM((2, 4, 8, C), F32),
            dma((n,)), dma((n,)), dma((n,)), dma((n,)),
            dma((2,)), dma((3,)), dma((TH // ROWS,)), dma((2, 8)), dma((2, 8)),
        ],
        compiler_params=pltpu.CompilerParams(
            collective_id=0, has_side_effects=True, vmem_limit_bytes=60 * 1024 * 1024
        ),
    )(
        features.reshape(n, CAP, F), cell_index.reshape(-1, 128), tile_rows, spread, w_in, w_dens.reshape(1, C),
        w_one.reshape(9 * C, C), w_two.reshape(9 * C, C),
    )


def solution(mesh):
    blocks = P(("lat", "lon"))
    in_specs = (P(("lat", "lon"), None), blocks, blocks, P(), P(), P(), P(), P())
    out_specs = P("lat", "lon", None)
    return jax.shard_map(shards, mesh=mesh, in_specs=in_specs, out_specs=out_specs, check_vma=False)
```

```python
import functools

import jax
import jax.numpy as jnp
from jax import lax
from jax.experimental import pallas as pl
from jax.experimental.pallas import tpu as pltpu
from jax.sharding import PartitionSpec as P

TH = 24
TW = 96
F = 128
C = 256
CAP = 96
PH = 26
PW = 98
PWP = 112
GROUP = 8
HALF = PH // 2
ROWS = 12
MESH = pl.DeviceIdType.MESH
F32 = jnp.float32
BF16 = jnp.bfloat16


def xor(a, b, count):
    out = 0
    bit = 1
    while bit < count:
        out = out + ((a // bit + b // bit) % 2) * bit
        bit *= 2
    return out


def kernel(
    lat_n, lon_n,
    feats, raw, used, spread, w_in, w_dens, w_one, w_two, out,
    cells, out_v, rows_in, cells_in, lhs, acc, mean, logd, grid_x, hid_x, win_v, wone_v, wtwo_v,
    row_out, row_in, col_out, col_in, corner_in,
    row_send, row_recv, cell_send, cell_recv, own_sem, w_sem, out_sem, halo_send, halo_recv,
):
    n = lat_n * lon_n
    groups = n // GROUP
    lat = lax.axis_index("lat")
    lon = lax.axis_index("lon")
    me = lat * lon_n + lon
    my_group = me // GROUP
    my_place = me % GROUP
    east = (lon + 1) % lon_n
    west = (lon + lon_n - 1) % lon_n

    barrier = pltpu.get_barrier_semaphore()

    @pl.loop(1, n)
    def _(k):
        peer = (me + k) % n
        pl.semaphore_signal(
            barrier, inc=1, device_id=(peer // lon_n, peer % lon_n), device_id_type=MESH
        )

    lane = lax.broadcasted_iota(jnp.int32, (1, 128), 1)

    @pl.loop(0, n // 4)
    def _(quad):
        one, two, three = (raw[pl.ds(3 * quad + k, 1)] for k in range(3))
        picks = [
            one,
            jnp.where(lane < 32, pltpu.roll(one, 32, 1), pltpu.roll(two, 32, 1)),
            jnp.where(lane < 64, pltpu.roll(two, 64, 1), pltpu.roll(three, 64, 1)),
            pltpu.roll(three, 96, 1),
        ]
        for k, pick in enumerate(picks):
            row = ((pick.astype(F32) + 0.5) * (1.0 / PW)).astype(jnp.int32)
            code = row * 128 + (pick - row * PW)
            cells[4 * quad + k] = jnp.where(lane < used[4 * quad + k], code, 127 * 128)

    own = [
        pltpu.make_async_copy(feats.at[me], rows_in.at[me], own_sem.at[0]),
        pltpu.make_async_copy(cells.at[me], cells_in.at[me], own_sem.at[1]),
    ]
    weights = [
        pltpu.make_async_copy(w_in, win_v, w_sem.at[0]),
        pltpu.make_async_copy(w_one, wone_v, w_sem.at[1]),
        pltpu.make_async_copy(w_two, wtwo_v, w_sem.at[2]),
    ]
    for item in weights:
        item.start()
    pl.semaphore_wait(barrier, n - 1)

    def row_copy(src_block, slot, peer):
        return pltpu.make_async_remote_copy(
            src_ref=feats.at[src_block], dst_ref=rows_in.at[slot],
            send_sem=row_send.at[src_block], recv_sem=row_recv.at[slot],
            device_id=(peer // lon_n, peer % lon_n), device_id_type=MESH,
        )

    def cell_copy(src_block, slot, peer):
        return pltpu.make_async_remote_copy(
            src_ref=cells.at[src_block], dst_ref=cells_in.at[slot],
            send_sem=cell_send.at[src_block], recv_sem=cell_recv.at[slot],
            device_id=(peer // lon_n, peer % lon_n), device_id_type=MESH,
        )

    def peer_of(step):
        turn = 1 + step // GROUP
        return xor(my_group, turn, groups) * GROUP + (my_place + step % GROUP) % GROUP

    def each_peer(act):
        for place in range(1, GROUP):
            act(my_group * GROUP + (my_place + place) % GROUP)

        @pl.loop(0, n - GROUP)
        def _(step):
            act(peer_of(step))

    def send(peer):
        cell_copy(peer, me, peer).start()
        row_copy(peer, me, peer).start()

    each_peer(send)
    for item in own:
        item.start()

    acc[...] = jnp.zeros_like(acc)

    def add_group(base):
        enc = jnp.concatenate([cells_in[base + m][:, :CAP] for m in range(GROUP)], axis=1)
        wide = GROUP * CAP
        col = jnp.broadcast_to(enc & 127, (PWP, wide))
        col_hot = jnp.where(
            lax.broadcasted_iota(jnp.int32, (PWP, wide), 0) == col, 1.0, 0.0
        ).astype(BF16)
        row = jnp.broadcast_to(enc >> 7, (16, wide))
        rows = rows_in[pl.ds(base, GROUP)].reshape(wide, F)
        rhs = jnp.concatenate([rows, jnp.ones((wide, C - F), BF16)], axis=1)
        col_hot = col_hot.reshape(PWP // 16, 16, wide)
        for r in range(PH):
            here = jnp.where(row == r, 1.0, 0.0).astype(BF16)
            lhs[r] = (col_hot * here[None]).reshape(PWP, wide)
        for half in range(2):
            span = slice(half * HALF, (half + 1) * HALF)
            part = jnp.dot(
                lhs[span].reshape(HALF * PWP, wide), rhs, preferred_element_type=F32
            )
            acc[span] += part.reshape(HALF, PWP, C)

    for place in range(1, GROUP):
        peer = my_group * GROUP + (my_place + place) % GROUP
        cell_copy(peer, peer, peer).wait_recv()
        row_copy(peer, peer, peer).wait_recv()
    for item in own:
        item.wait()
    add_group(my_group * GROUP)

    @pl.loop(1, groups)
    def _(step):
        base = xor(my_group, step, groups) * GROUP
        for m in range(GROUP):
            cell_copy(base + m, base + m, base + m).wait_recv()
            row_copy(base + m, base + m, base + m).wait_recv()
        add_group(base)

    weights[0].wait()

    def put(x_ref, stage, r, value):
        x_ref[r + 1, :, C : 2 * C] = value.astype(BF16)
        x_ref[r + 1, :, 0:C] = pltpu.roll(value, 1, 0).astype(BF16)
        x_ref[r + 1, :, 2 * C :] = pltpu.roll(value, TW - 1, 0).astype(BF16)
        col_out[stage, 0, pl.ds(r, 1)] = value[0:1]
        col_out[stage, 1, pl.ds(r, 1)] = value[TW - 1 : TW]

    @pl.loop(0, TH, unroll=2)
    def _(r):
        parts = []
        for b in range(3):
            parts.append(
                sum(spread[a, b] * acc[r + a, 0:104] for a in range(3))
            )
        total = parts[0][0:TW] + parts[1][1 : TW + 1] + parts[2][2 : TW + 2]
        level = 1.0 + total[:, F:]
        mean[r] = (total[:, :F] / level).astype(BF16)
        logd[r] = jnp.log(level)

    @pl.loop(0, TH // ROWS)
    def _(step):
        start = step * ROWS
        grid = jnp.dot(
            mean[pl.ds(start, ROWS)].reshape(ROWS * TW, F), win_v[...],
            preferred_element_type=F32,
        ).reshape(ROWS, TW, C)
        for k in range(ROWS):
            lg = logd[start + k]
            value = grid[k] + jnp.concatenate([lg, lg], axis=1) * w_dens[...]
            put(grid_x, 0, start + k, value)

    def halo_copy(stage, kind, src, dst, where):
        return pltpu.make_async_remote_copy(
            src_ref=src, dst_ref=dst,
            send_sem=halo_send.at[stage, kind], recv_sem=halo_recv.at[stage, kind],
            device_id=where, device_id_type=MESH,
        )

    def copies(stage, x_ref):
        up, down = lat - 1, lat + 1
        left, right = col_out.at[stage, 0], col_out.at[stage, 1]
        both = [
            halo_copy(stage, 0, right, col_in.at[stage, 0], (lat, east)),
            halo_copy(stage, 1, left, col_in.at[stage, 1], (lat, west)),
        ]
        low, high = pl.ds(0, 8), pl.ds(TH - 8, 8)
        to_up = [
            halo_copy(stage, 2, row_out.at[stage, 0], row_in.at[stage, 1], (up, lon)),
            halo_copy(stage, 3, right.at[low], corner_in.at[stage, 2], (up, east)),
            halo_copy(stage, 4, left.at[low], corner_in.at[stage, 3], (up, west)),
        ]
        to_down = [
            halo_copy(stage, 5, row_out.at[stage, 1], row_in.at[stage, 0], (down, lon)),
            halo_copy(stage, 6, right.at[high], corner_in.at[stage, 0], (down, east)),
            halo_copy(stage, 7, left.at[high], corner_in.at[stage, 1], (down, west)),
        ]
        return both, to_up, to_down

    def set_edges(x_ref, r, left, right):
        ids = lax.broadcasted_iota(jnp.int32, (16, C), 0)
        first = x_ref[r, 0:16, 0:C].astype(F32)
        x_ref[r, 0:16, 0:C] = jnp.where(ids == 0, left, first).astype(BF16)
        last = x_ref[r, TW - 16 : TW, 2 * C :].astype(F32)
        x_ref[r, TW - 16 : TW, 2 * C :] = jnp.where(ids == 15, right, last).astype(BF16)

    def exchange(stage, x_ref, beside):
        row_out[stage, 0] = x_ref[1, :, C : 2 * C]
        row_out[stage, 1] = x_ref[TH, :, C : 2 * C]
        both, to_up, to_down = copies(stage, x_ref)
        for item in both:
            item.start()

        @pl.when(lat > 0)
        def _():
            for item in to_up:
                item.start()

        @pl.when(lat < lat_n - 1)
        def _():
            for item in to_down:
                item.start()

        beside()
        for item in both:
            item.wait_recv()

        for r in range(TH):
            set_edges(
                x_ref, r + 1, col_in[stage, 0, r : r + 1], col_in[stage, 1, r : r + 1]
            )

        def outer(r, side, corner_row):
            value = row_in[stage, side].astype(F32)
            x_ref[r, :, C : 2 * C] = row_in[stage, side]
            x_ref[r, :, 0:C] = pltpu.roll(value, 1, 0).astype(BF16)
            x_ref[r, :, 2 * C :] = pltpu.roll(value, TW - 1, 0).astype(BF16)
            rows = slice(corner_row, corner_row + 1)
            set_edges(
                x_ref, r, corner_in[stage, 2 * side, rows], corner_in[stage, 2 * side + 1, rows]
            )

        @pl.when(lat > 0)
        def _():
            for item in to_down:
                item.wait_recv()
            outer(0, 0, 7)

        @pl.when(lat == 0)
        def _():
            x_ref[0] = jnp.zeros((TW, 3 * C), BF16)

        @pl.when(lat < lat_n - 1)
        def _():
            for item in to_up:
                item.wait_recv()
            outer(TH + 1, 1, 0)

        @pl.when(lat == lat_n - 1)
        def _():
            x_ref[TH + 1] = jnp.zeros((TW, 3 * C), BF16)

    def drain(stage, x_ref):
        both, to_up, to_down = copies(stage, x_ref)
        for item in both:
            item.wait_send()

        @pl.when(lat > 0)
        def _():
            for item in to_up:
                item.wait_send()

        @pl.when(lat < lat_n - 1)
        def _():
            for item in to_down:
                item.wait_send()

    def conv(x_ref, weight, start):
        window = jnp.concatenate(
            [x_ref[pl.ds(start + a, ROWS)].reshape(ROWS * TW, 3 * C) for a in range(3)], axis=1
        )
        return jnp.dot(window, weight[...], preferred_element_type=F32).reshape(ROWS, TW, C)

    def sent(peer):
        cell_copy(peer, me, peer).wait_send()
        row_copy(peer, me, peer).wait_send()

    exchange(0, grid_x, lambda: each_peer(sent))
    weights[1].wait()

    @pl.loop(0, TH // ROWS)
    def _(step):
        start = step * ROWS
        total = conv(grid_x, wone_v, start)
        for k in range(ROWS):
            value = total[k]
            put(hid_x, 1, start + k, value / (1.0 + jnp.exp(-value)))

    exchange(1, hid_x, lambda: None)
    weights[2].wait()

    def out_copy(start):
        span = pl.ds(start, ROWS)
        return pltpu.make_async_copy(out_v.at[span], out.at[span], out_sem.at[start // ROWS])

    @pl.loop(0, TH // ROWS)
    def _(step):
        start = step * ROWS
        total = conv(hid_x, wtwo_v, start)
        base = grid_x[pl.ds(start + 1, ROWS), :, C : 2 * C].astype(F32)
        out_v[pl.ds(start, ROWS)] = (base + total).astype(BF16)
        out_copy(start).start()

    drain(0, grid_x)
    drain(1, hid_x)
    for step in range(TH // ROWS):
        out_copy(step * ROWS).wait()


def shards(features, cell_index, tile_rows, spread, w_in, w_dens, w_one, w_two):
    lat_n = lax.axis_size("lat")
    lon_n = lax.axis_size("lon")
    n = lat_n * lon_n
    hbm = pl.BlockSpec(memory_space=pltpu.HBM)
    anywhere = pl.BlockSpec(memory_space=pl.ANY)
    vmem = pl.BlockSpec(memory_space=pltpu.VMEM)
    smem = pl.BlockSpec(memory_space=pltpu.SMEM)
    dma = pltpu.SemaphoreType.DMA
    return pl.pallas_call(
        functools.partial(kernel, lat_n, lon_n),
        out_shape=jax.ShapeDtypeStruct((TH, TW, C), BF16),
        in_specs=[hbm, vmem, smem, smem, hbm, vmem, hbm, hbm],
        out_specs=anywhere,
        scratch_shapes=[
            pltpu.VMEM((n, 1, 128), jnp.int32),
            pltpu.VMEM((TH, TW, C), BF16),
            pltpu.VMEM((n, CAP, F), BF16),
            pltpu.VMEM((n, 1, 128), jnp.int32),
            pltpu.VMEM((PH, PWP, GROUP * CAP), BF16),
            pltpu.VMEM((PH, PWP, C), F32),
            pltpu.VMEM((TH, TW, F), BF16),
            pltpu.VMEM((TH, TW, F), F32),
            pltpu.VMEM((TH + 2, TW, 3 * C), BF16),
            pltpu.VMEM((TH + 2, TW, 3 * C), BF16),
            pltpu.VMEM((F, C), BF16),
            pltpu.VMEM((9 * C, C), BF16),
            pltpu.VMEM((9 * C, C), BF16),
            pltpu.VMEM((2, 2, TW, C), BF16),
            pltpu.VMEM((2, 2, TW, C), BF16),
            pltpu.VMEM((2, 2, TH, C), F32),
            pltpu.VMEM((2, 2, TH, C), F32),
            pltpu.VMEM((2, 4, 8, C), F32),
            dma((n,)), dma((n,)), dma((n,)), dma((n,)),
            dma((2,)), dma((3,)), dma((TH // ROWS,)), dma((2, 8)), dma((2, 8)),
        ],
        compiler_params=pltpu.CompilerParams(
            collective_id=0, has_side_effects=True, vmem_limit_bytes=60 * 1024 * 1024
        ),
    )(
        features.reshape(n, CAP, F), cell_index.reshape(-1, 128), tile_rows, spread, w_in, w_dens.reshape(1, C),
        w_one.reshape(9 * C, C), w_two.reshape(9 * C, C),
    )


def solution(mesh):
    blocks = P(("lat", "lon"))
    in_specs = (P(("lat", "lon"), None), blocks, blocks, P(), P(), P(), P(), P())
    out_specs = P("lat", "lon", None)
    return jax.shard_map(shards, mesh=mesh, in_specs=in_specs, out_specs=out_specs, check_vma=False)
```
